128 devices in a mesh: seq: 16 (over z_lo, x, core), slate: 8 (over y, z_hi).
Axes of the slice: x: 4, y: 4, z: 4 (z_hi: 2, z_lo: 2; z = z_hi * 2 + z_lo), core: 2. Of those that a mesh axis runs over, the one named last changes fastest.
Arguments:
- features: bfloat16 [8, 12288, 512], P('slate', 'seq'), may hold values from -6 to 6
- user_ids: int32 [8], P('slate'), may hold values from 0 to 1023
- labels: int32 [8, 12288], P('slate', 'seq'), may hold values from 0 to 4, as said below
- user_table: bfloat16 [1024, 512], replicated, may hold values from -3 to 3
- gain_in: float32 [512], replicated, may hold values from 0.5 to 1.5
- w_query: bfloat16 [512, 512], replicated, may hold values from -0.75 to 0.75
- w_key: bfloat16 [512, 512], replicated, may hold values from -0.75 to 0.75
- w_value: bfloat16 [512, 512], replicated, may hold values from -0.25 to 0.25
- w_out: bfloat16 [512, 512], replicated, may hold values from -0.25 to 0.25
- gain_out: float32 [512], replicated, may hold values from 0.5 to 1.5
- w_score: float32 [512], replicated, may hold values from -0.25 to 0.25
Outputs:
- mixed: bfloat16 [8, 12288, 512], P('slate', 'seq')
- scores: float32 [8, 12288], P('slate', 'seq')
- loss: float32 [], replicated
The draws below stay inside these ranges and needn't reach their ends.
Inputs may be any that keep to these rules, and one draw needn't show every extreme that they name: `labels`: relevance grades of the items.
All inputs are finite; a program needn't handle non-finite values.
Results may differ from the reference program's by a relative error of at most 0.0045.
Values may be sent and summed in bfloat16 or wider, within the bound.
A program may use at most 192 MiB of HBM per device.

```python
import math
import jax
import jax.numpy as jnp
from jax import lax

D = 512
HEADS = 8
ITEM_DEV = 768
USERS = 1024
ITEMS = 12288
SLATES = 8


def draw_labels(key, part):
    position = jnp.arange(ITEMS, dtype=jnp.int32)
    upper = 2 + 4 * position // ITEMS
    upper = jnp.broadcast_to(upper[None, :], (SLATES, ITEMS))
    return jax.random.randint(jax.random.fold_in(key, 17), (SLATES, ITEMS), 0, upper, dtype=jnp.int32)


def plant(result, key, low, high):
    place = [jax.random.randint(jax.random.fold_in(key, axis), (), 0, length) for axis, length in enumerate(result.shape)]
    widest = result.shape.index(max(result.shape))
    next_to = place[:widest] + [(place[widest] + 1) % result.shape[widest]] + place[widest + 1:]
    return result.at[tuple(place)].set(low).at[tuple(next_to)].set(high)


def block_levels(key, dims, split, low, high):
    level, own = 1.0, jax.random.fold_in(key, 6)
    for dim, parts in split:
        heights = jnp.exp(jax.random.uniform(jax.random.fold_in(own, dim), (parts,), jnp.float32, low / len(split), high / len(split)))
        level = level * jnp.repeat(heights, dims[dim] // parts).reshape([-1 if axis == dim else 1 for axis in range(len(dims))])
    return level


def scatter_about(key, extent, deviation, reach, cuts=(), held_as=jnp.bfloat16):
    loudness = block_levels(key, extent, cuts, -0.22, 0.18) if cuts else 1.0
    entries = jax.random.normal(key, extent, jnp.float32) * deviation * loudness
    return jnp.minimum(jnp.maximum(entries, -reach), reach).astype(held_as)


def setup_inputs(seed: int = 0) -> dict:
    splits = jax.random.split(jax.random.key(seed), 12)
    features = scatter_about(splits[0], (SLATES, ITEMS, D), 1.0, 6.0, ((0, 8), (1, 16)))
    user_ids = plant(jax.random.randint(splits[1], (SLATES,), 0, USERS), jax.random.fold_in(splits[1], 1), 0, USERS - 1).astype(jnp.int32)
    labels = draw_labels(jax.random.fold_in(splits[11], 71), 0)
    user_table = scatter_about(splits[3], (USERS, D), 0.5, 3.0)
    gain_in = jnp.clip(1.0 + 0.1 * jax.random.normal(splits[4], (D,), jnp.float32), 0.5, 1.5)
    w_query = scatter_about(splits[5], (D, D), (D // 8) ** -0.5, 0.75)
    w_key = scatter_about(splits[6], (D, D), (D // 8) ** -0.5, 0.75)
    w_value = scatter_about(splits[7], (D, D), D ** -0.5, 0.25)
    w_out = scatter_about(splits[8], (D, D), D ** -0.5, 0.25)
    gain_out = jnp.clip(1.0 + 0.1 * jax.random.normal(splits[9], (D,), jnp.float32), 0.5, 1.5)
    w_score = scatter_about(splits[10], (D,), D ** -0.5, 0.25, (), jnp.float32)
    return dict(features=features, user_ids=user_ids, labels=labels, user_table=user_table, gain_in=gain_in, w_query=w_query, w_key=w_key, w_value=w_value, w_out=w_out, gain_out=gain_out, w_score=w_score)


soft_cap = 20.0
norm_eps = 1e-06

def rms_norm(inputs_row, gain_row):
    return inputs_row * lax.rsqrt(lax.optimization_barrier(jnp.mean(inputs_row * inputs_row, axis=-1, keepdims=True)) + norm_eps) * gain_row

def slate_pass(features, user_id, labels, user_table, gain_in, w_query, w_key, w_value, w_out, gain_out, w_score):
    item_rows = features.shape[0]
    model_width = features.shape[1]
    head_dim = model_width // HEADS
    score_scale = 1.0 / math.sqrt(head_dim)
    one_hot = (jnp.arange(user_table.shape[0], dtype=jnp.int32) == user_id).astype(jnp.bfloat16)[None, :]
    personal = jnp.dot(one_hot, user_table, preferred_element_type=jnp.float32)
    hidden = features.astype(jnp.float32) + personal
    normed = rms_norm(hidden, gain_in).astype(jnp.bfloat16)
    queries = jnp.dot(normed, w_query, preferred_element_type=jnp.float32).astype(jnp.bfloat16)
    keys_proj = jnp.dot(normed, w_key, preferred_element_type=jnp.float32).astype(jnp.bfloat16)
    values_proj = jnp.dot(normed, w_value, preferred_element_type=jnp.float32).astype(jnp.bfloat16)
    keys_all = keys_proj.reshape(item_rows, HEADS, head_dim).astype(jnp.float32)
    values_all = values_proj.reshape(item_rows, HEADS, head_dim).astype(jnp.float32)
    blocks = queries.reshape(item_rows // ITEM_DEV, ITEM_DEV, HEADS, head_dim)

    def attend(query_block):
        logits = jnp.einsum('qhd,khd->hqk', query_block.astype(jnp.float32), keys_all) * score_scale
        exp_scores = jnp.exp(soft_cap * jnp.tanh(logits / soft_cap))
        totals = lax.optimization_barrier(jnp.sum(exp_scores, axis=-1))
        rounded = lax.optimization_barrier(exp_scores.astype(jnp.bfloat16)).astype(jnp.float32)
        weighted = jnp.einsum('hqk,khd->qhd', rounded, values_all)
        return weighted / jnp.transpose(totals)[:, :, None]
    attended = lax.map(attend, blocks).reshape(item_rows, model_width).astype(jnp.bfloat16)
    mixed_sum = hidden + jnp.dot(attended, w_out, preferred_element_type=jnp.float32)
    out_normed = rms_norm(mixed_sum, gain_out)
    scored = lax.optimization_barrier(jnp.sum(out_normed * w_score, axis=-1))
    label_weight = jnp.exp(labels.astype(jnp.float32))
    partition = jnp.sum(jnp.exp(scored))
    slate_loss = jnp.log(partition / float(item_rows)) - jnp.sum(label_weight * scored) / jnp.sum(label_weight)
    return (mixed_sum.astype(jnp.bfloat16), scored, slate_loss)

def reference(features, user_ids, labels, user_table, gain_in, w_query, w_key, w_value, w_out, gain_out, w_score):

    def per_slate(inputs):
        return slate_pass(inputs[0], inputs[1], inputs[2], user_table, gain_in, w_query, w_key, w_value, w_out, gain_out, w_score)
    mixed, scores, losses = lax.map(per_slate, (features, user_ids, labels))
    return (mixed, scores, jnp.sum(losses))
```

```python
import math

import jax
import jax.numpy as jnp
from jax import lax
from jax.experimental import pallas as pl
from jax.experimental.pallas import tpu as pltpu
from jax.sharding import PartitionSpec as P

HEADS = 8
soft_cap = 20.0
norm_eps = 1e-06

bf16, f32 = jnp.bfloat16, jnp.float32
LOG2E = 1.4426950408889634
BLOCK = 256
AHEAD = 3


def sent_to_all(shard, axis):
    copies = jnp.broadcast_to(shard, (lax.axis_size(axis), *shard.shape))
    return lax.all_to_all(copies, axis, split_axis=0, concat_axis=0, tiled=True)


def taken_together(shard, axis):
    return sent_to_all(shard, axis).sum(axis=0)


def in_one(arrays, axis):
    ends = [0]
    for a in arrays:
        ends.append(ends[-1] + a.size)
    running = taken_together(jnp.concatenate([a.ravel() for a in arrays]), axis)
    return tuple((running[b:e].reshape(a.shape) for a, b, e in zip(arrays, ends, ends[1:])))


def rms_norm(inputs_row, gain_row):
    return (
        inputs_row
        * lax.rsqrt(jnp.mean(inputs_row * inputs_row, axis=-1, keepdims=True) + norm_eps)
        * gain_row
    )


def capped_weight(products):
    return jnp.exp2(jnp.tanh(products * (128.0 / 8 / soft_cap)) * (soft_cap * LOG2E))


def project_keys(rows, wk, k_ref):
    keys = jnp.dot(rows, wk, preferred_element_type=f32).astype(bf16)
    for pair in range(2):
        k_ref[pair] = keys[:, pair * 128 : (pair + 1) * 128]


def project_values(rows, wv_t, vt_ref):
    values_t = lax.dot_general(
        wv_t, rows, (((1,), (1,)), ((), ())), preferred_element_type=f32
    ).astype(bf16)
    for head in range(4):
        vt_ref[head, 0:64, :] = values_t[head * 64 : (head + 1) * 64]


def project_queries(rows, wq_t, qt_ref, at):
    queries_t = lax.dot_general(
        wq_t, rows, (((1,), (1,)), ((), ())), preferred_element_type=f32
    ).astype(bf16) * bf16(1.0 / 128)
    count = rows.shape[0]
    for head in range(4):
        mine, other = (head % 2) * 64, 64 - (head % 2) * 64
        qt_ref[head, mine : mine + 64, at : at + count] = queries_t[head * 64 : (head + 1) * 64]
        qt_ref[head, other : other + 64, at : at + count] = jnp.zeros((64, count), bf16)


def attend(k_ref, vt_ref, qt_ref, o_ref, heads, tiles):
    kts = k_ref.shape[1] // BLOCK
    work = [(h, t, b) for h in heads for t in tiles for b in range(kts)]
    ready = {}
    total = None
    for i in range(len(work) + AHEAD):
        if i < len(work):
            h, t, b = work[i]
            products = jnp.dot(
                k_ref[h // 2, b * BLOCK : (b + 1) * BLOCK],
                qt_ref[h, :, t * BLOCK : (t + 1) * BLOCK],
                preferred_element_type=f32,
            )
            ready[i] = capped_weight(products).astype(bf16)
        if i >= AHEAD:
            h, t, b = work[i - AHEAD]
            part = jnp.dot(
                vt_ref[h, :, b * BLOCK : (b + 1) * BLOCK],
                ready.pop(i - AHEAD),
                preferred_element_type=f32,
            )
            total = part if b == 0 else total + part
            if b == kts - 1:
                o_ref[h, :, t * BLOCK : (t + 1) * BLOCK] += total


def attention_kernel(own_ref, seg_ref, wq_ref, wk_ref, wv_ref, out_ref, k_ref, vt_ref, qt_ref, o_ref):
    step = pl.program_id(0)

    @pl.when(step == 0)
    def _():
        o_ref[...] = jnp.zeros_like(o_ref)
        row = lax.broadcasted_iota(jnp.int32, (16, vt_ref.shape[2]), 0)
        for head in range(4):
            vt_ref[head, 64:80, :] = jnp.where(row == 0, 1.0, 0.0).astype(bf16)
        for t in range(own_ref.shape[0] // BLOCK):
            project_queries(own_ref[t * BLOCK : (t + 1) * BLOCK], wq_ref[...], qt_ref, t * BLOCK)

    project_keys(seg_ref[...], wk_ref[...], k_ref)
    project_values(seg_ref[...], wv_ref[...], vt_ref)
    attend(k_ref, vt_ref, qt_ref, o_ref, range(4), range(qt_ref.shape[2] // BLOCK))

    @pl.when(step == pl.num_programs(0) - 1)
    def _():
        for head in range(4):
            out_ref[head * 64 : (head + 1) * 64] = (
                o_ref[head, 0:64] / o_ref[head, 64:65]
            ).astype(bf16)


def attention(own, seg, wq_t, wk, wv_t, rows):
    queries, width = own.shape
    chunks = seg.shape[0] // rows
    whole = lambda shape: pl.BlockSpec(shape, lambda i: (0, 0))
    return pl.pallas_call(
        attention_kernel,
        grid=(chunks,),
        out_shape=jax.ShapeDtypeStruct((width // 2, queries), bf16),
        in_specs=[
            whole(own.shape),
            pl.BlockSpec((rows, width), lambda i: (i, 0)),
            whole(wq_t.shape),
            whole(wk.shape),
            whole(wv_t.shape),
        ],
        out_specs=whole((width // 2, queries)),
        scratch_shapes=[
            pltpu.VMEM((2, rows, 128), bf16),
            pltpu.VMEM((4, 80, rows), bf16),
            pltpu.VMEM((4, 128, queries), bf16),
            pltpu.VMEM((4, 80, queries), f32),
        ],
        compiler_params=pltpu.CompilerParams(vmem_limit_bytes=48 * 2**20),
        name="attention",
    )(own, seg, wq_t, wk, wv_t)


def shards(
    features,
    user_ids,
    labels,
    user_table,
    gain_in,
    w_query,
    w_key,
    w_value,
    w_out,
    gain_out,
    w_score,
):
    local_items = features[0]
    item_rows, model_width = local_items.shape
    half = model_width // 2
    ring = lax.axis_size("seq")
    slate_items = float(item_rows * ring)
    me = lax.axis_index("seq")
    core = me % 2
    personal = lax.dynamic_slice_in_dim(user_table, user_ids[0], 1, 0)
    hidden = local_items.astype(f32) + personal.astype(f32)
    normed = rms_norm(hidden, gain_in).astype(bf16)
    segment = lax.all_gather(normed, "seq", axis=0, tiled=True)
    cut = lambda w: lax.dynamic_slice_in_dim(w, core * half, half, 1)
    own = lax.dynamic_slice_in_dim(segment, (me - core) * item_rows, 2 * item_rows, 0)
    mine_t = attention(own, segment, cut(w_query).T, cut(w_key), cut(w_value).T, item_rows)
    kept = lax.dynamic_slice_in_dim(mine_t, core * item_rows, item_rows, 1)
    given = lax.dynamic_slice_in_dim(mine_t, (1 - core) * item_rows, item_rows, 1)
    got = lax.ppermute(given, "seq", [(i, i ^ 1) for i in range(ring)])
    attended_t = jnp.where(
        core == 0, jnp.concatenate([kept, got], 0), jnp.concatenate([got, kept], 0)
    )
    mixed_sum = hidden + lax.dot_general(
        attended_t, w_out, (((0,), (0,)), ((), ())), preferred_element_type=f32
    )
    out_normed = rms_norm(mixed_sum, gain_out)
    scored = jnp.sum(out_normed * w_score, axis=-1)
    label_weight = jnp.exp(labels[0].astype(f32))
    exp_part = jnp.sum(jnp.exp(scored))
    weight_part = jnp.sum(label_weight)
    product_part = jnp.sum(label_weight * scored)
    partition, weight_sum, weighted_score = in_one((exp_part, weight_part, product_part), "seq")
    total_loss = taken_together(
        jnp.log(partition / slate_items) - weighted_score / weight_sum, "slate"
    )
    return (mixed_sum.astype(bf16)[None], scored[None], total_loss)


def solution(mesh):
    return jax.shard_map(
        shards,
        mesh=mesh,
        in_specs=(
            P("slate", "seq", None),
            P("slate"),
            P("slate", "seq"),
            P(),
            P(),
            P(),
            P(),
            P(),
            P(),
            P(),
            P(),
        ),
        out_specs=(P("slate", "seq", None), P("slate", "seq"), P()),
        check_vma=False,
    )
```

```python
import functools

import jax
import jax.numpy as jnp
from jax import lax
from jax.experimental import pallas as pl
from jax.experimental.pallas import tpu as pltpu
from jax.sharding import PartitionSpec as P

HEADS = 8
soft_cap = 20.0
norm_eps = 1e-06

bf16, f32 = jnp.bfloat16, jnp.float32
LOG2E = 1.4426950408889634
BLOCK = 256
AHEAD = 3
MESH = pl.DeviceIdType.MESH


def capped_weight(products):
    return jnp.exp2(jnp.tanh(products * (128.0 / 8 / soft_cap)) * (soft_cap * LOG2E))


def project_keys(rows, wk, k_ref):
    keys = jnp.dot(rows, wk, preferred_element_type=f32).astype(bf16)
    for pair in range(2):
        k_ref[pair] = keys[:, pair * 128 : (pair + 1) * 128]


def project_values(rows, wv_t, vt_ref):
    values_t = lax.dot_general(
        wv_t, rows, (((1,), (1,)), ((), ())), preferred_element_type=f32
    ).astype(bf16)
    for head in range(4):
        vt_ref[head, 0:64, :] = values_t[head * 64 : (head + 1) * 64]


def project_queries(rows, wq_t, qt_ref, at):
    queries_t = lax.dot_general(
        wq_t, rows, (((1,), (1,)), ((), ())), preferred_element_type=f32
    ).astype(bf16) * bf16(1.0 / 128)
    count = rows.shape[0]
    for head in range(4):
        mine, other = (head % 2) * 64, 64 - (head % 2) * 64
        qt_ref[head, mine : mine + 64, at : at + count] = queries_t[head * 64 : (head + 1) * 64]
        qt_ref[head, other : other + 64, at : at + count] = jnp.zeros((64, count), bf16)


def attend(k_ref, vt_ref, qt_ref, o_ref, heads, tiles):
    kts = k_ref.shape[1] // BLOCK
    work = [(h, t, b) for h in heads for t in tiles for b in range(kts)]
    ready = {}
    total = None
    for i in range(len(work) + AHEAD):
        if i < len(work):
            h, t, b = work[i]
            products = jnp.dot(
                k_ref[h // 2, b * BLOCK : (b + 1) * BLOCK],
                qt_ref[h, :, t * BLOCK : (t + 1) * BLOCK],
                preferred_element_type=f32,
            )
            ready[i] = capped_weight(products).astype(bf16)
        if i >= AHEAD:
            h, t, b = work[i - AHEAD]
            part = jnp.dot(
                vt_ref[h, :, b * BLOCK : (b + 1) * BLOCK],
                ready.pop(i - AHEAD),
                preferred_element_type=f32,
            )
            total = part if b == 0 else total + part
            if b == kts - 1:
                o_ref[h, :, t * BLOCK : (t + 1) * BLOCK] += total


def rms_scale(rows):
    return lax.rsqrt(jnp.mean(rows * rows, axis=-1, keepdims=True) + norm_eps)


def fused_kernel(
    seq,
    slates,
    features_ref,
    personal_ref,
    labels_ref,
    gain_in_ref,
    wq_ref,
    wk_ref,
    wv_ref,
    wo_ref,
    gain_out_ref,
    w_score_ref,
    mixed_ref,
    scores_ref,
    loss_ref,
    x_ref,
    k_ref,
    vt_ref,
    qt_ref,
    o_ref,
    give_ref,
    att_ref,
    wvt_ref,
    parts_ref,
    losses_ref,
    send_sem,
    recv_sem,
    parts_send,
    parts_recv,
    losses_send,
    losses_recv,
):
    rows, width = features_ref.shape
    half = width // 2
    third = rows // 3
    me = lax.axis_index("seq")
    my_slate = lax.axis_index("slate")
    core, x, z = lax.rem(me, 2), lax.rem(lax.div(me, 2), 4), lax.div(me, 8)
    at = lambda zz, xx, cc: (zz * 4 + xx) * 2 + cc
    right = at(z, lax.rem(x + 1, 4), core)
    left = at(z, lax.rem(x + 3, 4), core)
    across = at(1 - z, x, core)
    partner = at(z, x, 1 - core)

    barrier = pltpu.get_barrier_semaphore()
    for k in range(1, seq):
        pl.semaphore_signal(
            barrier, inc=1, device_id={"seq": lax.rem(me + k, seq)}, device_id_type=MESH
        )
    for k in range(1, slates):
        pl.semaphore_signal(
            barrier, inc=1, device_id={"slate": lax.rem(my_slate + k, slates)}, device_id_type=MESH
        )

    for t in range(3):
        tile = slice(t * third, (t + 1) * third)
        hidden = features_ref[tile].astype(f32) + personal_ref[...].astype(f32)
        x_ref[0, tile] = (hidden * rms_scale(hidden) * gain_in_ref[...]).astype(bf16)

    copies = {}

    def piece(group, part):
        return x_ref.at[group, part * third : (part + 1) * third]

    def copy(name, source, target, device):
        index = len(copies)
        copies[name] = pltpu.make_async_remote_copy(
            src_ref=source,
            dst_ref=target,
            send_sem=send_sem.at[index],
            recv_sem=recv_sem.at[index],
            device_id={"seq": device},
            device_id_type=MESH,
        )

    copy("own", x_ref.at[0], x_ref.at[1], partner)
    for p in range(3):
        copy(f"a{p}", piece(0, p), piece(2 + p, 0), across)
        copy(f"l{p}", piece(0, p), piece(2 + p, 1), right)
        copy(f"r{p}", piece(0, p), piece(2 + p, 2), left)
        copy(f"al{p}", piece(2 + p, 0), piece(8 + p, 1), right)
        copy(f"ar{p}", piece(2 + p, 0), piece(8 + p, 2), left)
        if p != 1:
            copy(f"o{p}", piece(2 + p, 1), piece(8 + p, 0), right)
        else:
            copy(f"o{p}", piece(2 + p, 2), piece(8 + p, 0), left)
        copy(f"ao{p}", piece(8 + p, 0), piece(14, p), across)
        copy(f"m{p}", x_ref.at[2 + p], x_ref.at[5 + p], partner)
        copy(f"n{p}", x_ref.at[8 + p], x_ref.at[11 + p], partner)
    copy("last", x_ref.at[14], x_ref.at[15], partner)
    copy("swap", give_ref, att_ref.at[core], partner)

    def start(*names):
        for name in names:
            copies[name].start()

    def arrived(*names):
        for name in names:
            copies[name].wait_recv()

    pl.semaphore_wait(barrier, seq - 1 + slates - 1)
    start("own")
    for p in range(3):
        start(f"a{p}", f"l{p}", f"r{p}")

    columns = pl.ds(pl.multiple_of(core * half, half), half)
    wq_t = wq_ref[:, columns].T
    wvt_ref[...] = wv_ref[:, columns].T
    row = lax.broadcasted_iota(jnp.int32, (16, rows), 0)
    for head in range(4):
        vt_ref[head, 64:80, :] = jnp.where(row == 0, 1.0, 0.0).astype(bf16)
    o_ref[...] = jnp.zeros_like(o_ref)
    project_queries(x_ref[0], wq_t, qt_ref, 0)
    arrived("own")
    project_queries(x_ref[1], wq_t, qt_ref, rows)

    def group(g, carry):
        for p in range(3):

            @pl.when(g == 2 + p)
            def _():
                arrived(f"a{p}", f"l{p}", f"r{p}")
                start(f"al{p}", f"ar{p}", f"o{p}", f"m{p}")

            @pl.when(g == 5 + p)
            def _():
                arrived(f"m{p}")

            @pl.when(g == 7)
            def _():
                arrived(f"o{p}")
                start(f"ao{p}")

            @pl.when(g == 8 + p)
            def _():
                arrived(f"al{p}", f"ar{p}")
                start(f"n{p}")

            @pl.when(g == 11 + p)
            def _():
                arrived(f"n{p}")

        @pl.when(g == 14)
        def _():
            arrived("ao0", "ao1", "ao2")
            start("last")

        @pl.when(g == 15)
        def _():
            arrived("last")

        project_keys(x_ref[g], wk_ref[:, columns], k_ref)
        project_values(x_ref[g], wvt_ref[...], vt_ref)
        attend(k_ref, vt_ref, qt_ref, o_ref, range(4), range(qt_ref.shape[2] // BLOCK))
        return carry

    lax.fori_loop(0, seq, group, 0)

    def finished(head, first):
        span = slice(first, first + rows)
        return (o_ref[head, 0:64, span] / o_ref[head, 64:65, span]).astype(bf16)

    for head in range(4):
        give_ref[head * 64 : (head + 1) * 64] = finished(head, rows)
    start("swap")
    for head in range(4):
        att_ref[core, head * 64 : (head + 1) * 64] = finished(head, 0)
    arrived("swap")

    sums = [jnp.zeros((1, third), f32)] * 3
    for t in range(3):
        tile = slice(t * third, (t + 1) * third)
        hidden = features_ref[tile].astype(f32) + personal_ref[...].astype(f32)
        mixed = hidden
        for c in range(2):
            mixed = mixed + lax.dot_general(
                att_ref[c, :, tile],
                wo_ref[c * half : (c + 1) * half],
                (((0,), (0,)), ((), ())),
                preferred_element_type=f32,
            )
        mixed_ref[tile] = mixed.astype(bf16)
        scored = jnp.sum(
            mixed * rms_scale(mixed) * gain_out_ref[...] * w_score_ref[...], axis=-1, keepdims=True
        )
        scored = jnp.broadcast_to(scored, (third, 128)).T[0:1]
        scores_ref[:, tile] = scored
        weight = jnp.exp(labels_ref[:, tile].astype(f32))
        terms = (jnp.exp(scored), weight, weight * scored)
        sums = [total + term for total, term in zip(sums, terms)]

    def shared(tile, buffer, sends, recvs, axis, mine, count):
        buffer[mine] = tile
        sent = []
        for k in range(1, count):
            sent.append(
                pltpu.make_async_remote_copy(
                    src_ref=buffer.at[mine],
                    dst_ref=buffer.at[mine],
                    send_sem=sends.at[k],
                    recv_sem=recvs.at[mine],
                    device_id={axis: lax.rem(mine + k, count)},
                    device_id_type=MESH,
                )
            )
            sent[-1].start()
        for k in range(1, count):
            other = lax.rem(mine + k, count)
            pltpu.make_async_remote_copy(
                src_ref=buffer.at[other],
                dst_ref=buffer.at[other],
                send_sem=sends.at[k],
                recv_sem=recvs.at[other],
                device_id={axis: other},
                device_id_type=MESH,
            ).wait_recv()
        total = buffer[0]
        for k in range(1, count):
            total = total + buffer[k]
        for one in sent:
            one.wait_send()
        return total

    row = lax.broadcasted_iota(jnp.int32, (8, 128), 0)
    tile = jnp.zeros((8, 128), f32)
    for i, total in enumerate(sums):
        tile = jnp.where(row == i, jnp.sum(total, axis=-1, keepdims=True), tile)
    tile = shared(tile, parts_ref, parts_send, parts_recv, "seq", me, seq)
    slate_loss = jnp.log(tile[0:1] / float(rows * seq)) - tile[2:3] / tile[1:2]
    slate_loss = jnp.broadcast_to(slate_loss, (8, 128))
    loss_ref[...] = shared(
        slate_loss, losses_ref, losses_send, losses_recv, "slate", my_slate, slates
    )
    for one in copies.values():
        one.wait_send()


def shards(
    features,
    user_ids,
    labels,
    user_table,
    gain_in,
    w_query,
    w_key,
    w_value,
    w_out,
    gain_out,
    w_score,
):
    _, rows, width = features.shape
    seq, slates = lax.axis_size("seq"), lax.axis_size("slate")
    personal = lax.dynamic_slice_in_dim(user_table, user_ids[0], 1, 0)
    vmem = pl.BlockSpec(memory_space=pltpu.VMEM)
    mixed, scores, loss = pl.pallas_call(
        functools.partial(fused_kernel, seq, slates),
        out_shape=(
            jax.ShapeDtypeStruct((rows, width), bf16),
            jax.ShapeDtypeStruct((1, rows), f32),
            jax.ShapeDtypeStruct((8, 128), f32),
        ),
        in_specs=[vmem] * 10,
        out_specs=(vmem, vmem, vmem),
        scratch_shapes=[
            pltpu.VMEM((seq, rows, width), bf16),
            pltpu.VMEM((2, rows, 128), bf16),
            pltpu.VMEM((4, 80, rows), bf16),
            pltpu.VMEM((4, 128, 2 * rows), bf16),
            pltpu.VMEM((4, 80, 2 * rows), f32),
            pltpu.VMEM((width // 2, rows), bf16),
            pltpu.VMEM((2, width // 2, rows), bf16),
            pltpu.VMEM((width // 2, width), bf16),
            pltpu.VMEM((seq, 8, 128), f32),
            pltpu.VMEM((slates, 8, 128), f32),
            pltpu.SemaphoreType.DMA((30,)),
            pltpu.SemaphoreType.DMA((30,)),
            pltpu.SemaphoreType.DMA((seq,)),
            pltpu.SemaphoreType.DMA((seq,)),
            pltpu.SemaphoreType.DMA((slates,)),
            pltpu.SemaphoreType.DMA((slates,)),
        ],
        compiler_params=pltpu.CompilerParams(
            collective_id=0, has_side_effects=True, vmem_limit_bytes=56 * 2**20
        ),
        name="slate_attention",
    )(
        features[0],
        personal,
        labels,
        gain_in[None],
        w_query,
        w_key,
        w_value,
        w_out,
        gain_out[None],
        w_score[None],
    )
    return (mixed[None], scores, loss[0, 0])


def solution(mesh):
    return jax.shard_map(
        shards,
        mesh=mesh,
        in_specs=(
            P("slate", "seq", None),
            P("slate"),
            P("slate", "seq"),
            P(),
            P(),
            P(),
            P(),
            P(),
            P(),
            P(),
            P(),
        ),
        out_specs=(P("slate", "seq", None), P("slate", "seq"), P()),
        check_vma=False,
    )
```

```python
import functools

import jax
import jax.numpy as jnp
from jax import lax
from jax.experimental import pallas as pl
from jax.experimental.pallas import tpu as pltpu
from jax.sharding import PartitionSpec as P

HEADS = 8
soft_cap = 20.0
norm_eps = 1e-06

bf16, f32 = jnp.bfloat16, jnp.float32
LOG2E = 1.4426950408889634
BLOCK = 256
AHEAD = 3
MESH = pl.DeviceIdType.MESH


def capped_weight(products):
    return jnp.exp2(jnp.tanh(products * (128.0 / 8 / soft_cap)) * (soft_cap * LOG2E))


def project_keys(rows, wk, k_ref):
    keys = jnp.dot(rows, wk, preferred_element_type=f32).astype(bf16)
    for pair in range(2):
        k_ref[pair] = keys[:, pair * 128 : (pair + 1) * 128]


def project_values(rows, wv_t, vt_ref):
    values_t = lax.dot_general(
        wv_t, rows, (((1,), (1,)), ((), ())), preferred_element_type=f32
    ).astype(bf16)
    for head in range(4):
        vt_ref[head, 0:64, :] = values_t[head * 64 : (head + 1) * 64]


def project_queries(rows, wq_t, qt_ref, at):
    queries_t = lax.dot_general(
        wq_t, rows, (((1,), (1,)), ((), ())), preferred_element_type=f32
    ).astype(bf16) * bf16(1.0 / 128)
    count = rows.shape[0]
    for head in range(4):
        mine, other = (head % 2) * 64, 64 - (head % 2) * 64
        qt_ref[head, mine : mine + 64, at : at + count] = queries_t[head * 64 : (head + 1) * 64]
        qt_ref[head, other : other + 64, at : at + count] = jnp.zeros((64, count), bf16)


def attend(k_refs, vt_refs, qt_ref, o_ref, heads, tiles):
    kts = k_refs[0].shape[1] // BLOCK
    work = [(g, h, t, b) for g in range(2) for h in heads for t in tiles for b in range(kts)]
    ready = {}
    total = None
    for i in range(len(work) + AHEAD):
        if i < len(work):
            g, h, t, b = work[i]
            products = jnp.dot(
                k_refs[g][h // 2, b * BLOCK : (b + 1) * BLOCK],
                qt_ref[h, :, t * BLOCK : (t + 1) * BLOCK],
                preferred_element_type=f32,
            )
            ready[i] = capped_weight(products).astype(bf16)
        if i >= AHEAD:
            g, h, t, b = work[i - AHEAD]
            part = jnp.dot(
                vt_refs[g][h, :, b * BLOCK : (b + 1) * BLOCK],
                ready.pop(i - AHEAD),
                preferred_element_type=f32,
            )
            total = part if b == 0 else total + part
            if b == kts - 1:
                o_ref[h, :, t * BLOCK : (t + 1) * BLOCK] += total


def rms_scale(rows):
    return lax.rsqrt(jnp.mean(rows * rows, axis=-1, keepdims=True) + norm_eps)


def fused_kernel(
    seq,
    slates,
    features_ref,
    personal_ref,
    labels_ref,
    gain_in_ref,
    wq_ref,
    wk_ref,
    wv_ref,
    wo_ref,
    gain_out_ref,
    w_score_ref,
    mixed_ref,
    scores_ref,
    loss_ref,
    x_ref,
    k_a_ref,
    k_b_ref,
    vt_a_ref,
    vt_b_ref,
    qt_ref,
    o_ref,
    give_ref,
    att_ref,
    wvt_ref,
    parts_ref,
    losses_ref,
    send_sem,
    recv_sem,
    parts_send,
    parts_recv,
    losses_send,
    losses_recv,
):
    rows, width = features_ref.shape
    half = width // 2
    third = rows // 3
    me = lax.axis_index("seq")
    my_slate = lax.axis_index("slate")
    core, x, z = lax.rem(me, 2), lax.rem(lax.div(me, 2), 4), lax.div(me, 8)
    at = lambda zz, xx, cc: (zz * 4 + xx) * 2 + cc
    right = at(z, lax.rem(x + 1, 4), core)
    left = at(z, lax.rem(x + 3, 4), core)
    across = at(1 - z, x, core)
    partner = at(z, x, 1 - core)

    barrier = pltpu.get_barrier_semaphore()
    for k in range(1, seq):
        pl.semaphore_signal(
            barrier, inc=1, device_id={"seq": lax.rem(me + k, seq)}, device_id_type=MESH
        )
    for k in range(1, slates):
        pl.semaphore_signal(
            barrier, inc=1, device_id={"slate": lax.rem(my_slate + k, slates)}, device_id_type=MESH
        )

    for t in range(3):
        tile = slice(t * third, (t + 1) * third)
        hidden = features_ref[tile].astype(f32) + personal_ref[...].astype(f32)
        x_ref[0, tile] = (hidden * rms_scale(hidden) * gain_in_ref[...]).astype(bf16)

    copies = {}

    def piece(group, part):
        return x_ref.at[group, part * third : (part + 1) * third]

    def copy(name, source, target, device):
        index = len(copies)
        copies[name] = pltpu.make_async_remote_copy(
            src_ref=source,
            dst_ref=target,
            send_sem=send_sem.at[index],
            recv_sem=recv_sem.at[index],
            device_id={"seq": device},
            device_id_type=MESH,
        )

    copy("own", x_ref.at[0], x_ref.at[1], partner)
    for p in range(3):
        copy(f"a{p}", piece(0, p), piece(2 + p, 0), across)
        copy(f"l{p}", piece(0, p), piece(2 + p, 1), right)
        copy(f"r{p}", piece(0, p), piece(2 + p, 2), left)
        copy(f"al{p}", piece(2 + p, 0), piece(8 + p, 1), right)
        copy(f"ar{p}", piece(2 + p, 0), piece(8 + p, 2), left)
        if p != 1:
            copy(f"o{p}", piece(2 + p, 1), piece(8 + p, 0), right)
        else:
            copy(f"o{p}", piece(2 + p, 2), piece(8 + p, 0), left)
        copy(f"ao{p}", piece(8 + p, 0), piece(14, p), across)
        copy(f"m{p}", x_ref.at[2 + p], x_ref.at[5 + p], partner)
        copy(f"n{p}", x_ref.at[8 + p], x_ref.at[11 + p], partner)
    copy("last", x_ref.at[14], x_ref.at[15], partner)
    copy("swap", give_ref, att_ref.at[core], partner)

    def start(*names):
        for name in names:
            copies[name].start()

    def arrived(*names):
        for name in names:
            copies[name].wait_recv()

    pl.semaphore_wait(barrier, seq - 1 + slates - 1)
    start("own")
    for p in range(3):
        start(f"a{p}", f"l{p}", f"r{p}")

    columns = pl.ds(pl.multiple_of(core * half, half), half)
    wq_t = wq_ref[:, columns].T
    wvt_ref[...] = wv_ref[:, columns].T
    row = lax.broadcasted_iota(jnp.int32, (16, rows), 0)
    k_refs, vt_refs = (k_a_ref, k_b_ref), (vt_a_ref, vt_b_ref)
    for vt_ref, head in [(v, h) for v in vt_refs for h in range(4)]:
        vt_ref[head, 64:80, :] = jnp.where(row == 0, 1.0, 0.0).astype(bf16)
    o_ref[...] = jnp.zeros_like(o_ref)
    project_queries(x_ref[0], wq_t, qt_ref, 0)
    arrived("own")
    project_queries(x_ref[1], wq_t, qt_ref, rows)

    def pair(i, carry):
        @pl.when(i == 1)
        def _():
            for p in (0, 1):
                arrived(f"a{p}", f"l{p}", f"r{p}")
                start(f"al{p}", f"ar{p}", f"o{p}", f"m{p}")

        @pl.when(i == 2)
        def _():
            arrived("a2", "l2", "r2", "m0")
            start("al2", "ar2", "o2", "m2")

        @pl.when(i == 3)
        def _():
            arrived("m1", "m2")
            for p in (0, 1):
                arrived(f"o{p}")
                start(f"ao{p}")

        @pl.when(i == 4)
        def _():
            for p in (0, 1):
                arrived(f"al{p}", f"ar{p}")
                start(f"n{p}")
            arrived("o2")
            start("ao2")

        @pl.when(i == 5)
        def _():
            arrived("al2", "ar2", "n0")
            start("n2")

        @pl.when(i == 6)
        def _():
            arrived("n1", "n2", "ao0", "ao1", "ao2")
            start("last")

        @pl.when(i == 7)
        def _():
            arrived("last")

        for b in range(2):
            project_keys(x_ref[2 * i + b], wk_ref[:, columns], k_refs[b])
            project_values(x_ref[2 * i + b], wvt_ref[...], vt_refs[b])
        tiles = range(qt_ref.shape[2] // BLOCK)
        attend(k_refs, vt_refs, qt_ref, o_ref, range(4), tiles)
        return carry

    lax.fori_loop(0, seq // 2, pair, 0)

    def finished(head, first):
        span = slice(first, first + rows)
        return (o_ref[head, 0:64, span] * (1.0 / o_ref[head, 64:65, span])).astype(bf16)

    for head in range(4):
        give_ref[head * 64 : (head + 1) * 64] = finished(head, rows)
    start("swap")
    for head in range(4):
        att_ref[core, head * 64 : (head + 1) * 64] = finished(head, 0)
    arrived("swap")

    sums = [jnp.zeros((1, third), f32)] * 3
    for t in range(3):
        tile = slice(t * third, (t + 1) * third)
        hidden = features_ref[tile].astype(f32) + personal_ref[...].astype(f32)
        mixed = hidden
        for c in range(2):
            mixed = mixed + lax.dot_general(
                att_ref[c, :, tile],
                wo_ref[c * half : (c + 1) * half],
                (((0,), (0,)), ((), ())),
                preferred_element_type=f32,
            )
        mixed_ref[tile] = mixed.astype(bf16)
        scored = jnp.sum(
            mixed * rms_scale(mixed) * gain_out_ref[...] * w_score_ref[...], axis=-1, keepdims=True
        )
        scored = jnp.broadcast_to(scored, (third, 128)).T[0:1]
        scores_ref[:, tile] = scored
        weight = jnp.exp(labels_ref[:, tile].astype(f32))
        terms = (jnp.exp(scored), weight, weight * scored)
        sums = [total + term for total, term in zip(sums, terms)]

    def shared(tile, buffer, sends, recvs, axis, mine, count):
        buffer[mine] = tile
        sent = []
        for k in range(1, count):
            sent.append(
                pltpu.make_async_remote_copy(
                    src_ref=buffer.at[mine],
                    dst_ref=buffer.at[mine],
                    send_sem=sends.at[k],
                    recv_sem=recvs.at[mine],
                    device_id={axis: lax.rem(mine + k, count)},
                    device_id_type=MESH,
                )
            )
            sent[-1].start()
        for k in range(1, count):
            other = lax.rem(mine + k, count)
            pltpu.make_async_remote_copy(
                src_ref=buffer.at[other],
                dst_ref=buffer.at[other],
                send_sem=sends.at[k],
                recv_sem=recvs.at[other],
                device_id={axis: other},
                device_id_type=MESH,
            ).wait_recv()
        total = buffer[0]
        for k in range(1, count):
            total = total + buffer[k]
        for one in sent:
            one.wait_send()
        return total

    row = lax.broadcasted_iota(jnp.int32, (8, 128), 0)
    tile = jnp.zeros((8, 128), f32)
    for i, total in enumerate(sums):
        tile = jnp.where(row == i, jnp.sum(total, axis=-1, keepdims=True), tile)
    tile = shared(tile, parts_ref, parts_send, parts_recv, "seq", me, seq)
    slate_loss = jnp.log(tile[0:1] / float(rows * seq)) - tile[2:3] / tile[1:2]
    slate_loss = jnp.broadcast_to(slate_loss, (8, 128))
    loss_ref[...] = shared(
        slate_loss, losses_ref, losses_send, losses_recv, "slate", my_slate, slates
    )[0:1, 0:1]
    for one in copies.values():
        one.wait_send()


def shards(
    features,
    user_ids,
    labels,
    user_table,
    gain_in,
    w_query,
    w_key,
    w_value,
    w_out,
    gain_out,
    w_score,
):
    _, rows, width = features.shape
    seq, slates = lax.axis_size("seq"), lax.axis_size("slate")
    personal = lax.dynamic_slice_in_dim(user_table, user_ids[0], 1, 0)
    vmem = pl.BlockSpec(memory_space=pltpu.VMEM)
    mixed, scores, loss = pl.pallas_call(
        functools.partial(fused_kernel, seq, slates),
        out_shape=(
            pltpu.VMEM((rows, width), bf16),
            pltpu.VMEM((1, rows), f32),
            jax.ShapeDtypeStruct((1, 1), f32),
        ),
        in_specs=[vmem] * 10,
        out_specs=(vmem, vmem, vmem),
        scratch_shapes=[
            pltpu.VMEM((seq, rows, width), bf16),
            pltpu.VMEM((2, rows, 128), bf16),
            pltpu.VMEM((2, rows, 128), bf16),
            pltpu.VMEM((4, 80, rows), bf16),
            pltpu.VMEM((4, 80, rows), bf16),
            pltpu.VMEM((4, 128, 2 * rows), bf16),
            pltpu.VMEM((4, 80, 2 * rows), f32),
            pltpu.VMEM((width // 2, rows), bf16),
            pltpu.VMEM((2, width // 2, rows), bf16),
            pltpu.VMEM((width // 2, width), bf16),
            pltpu.VMEM((seq, 8, 128), f32),
            pltpu.VMEM((slates, 8, 128), f32),
            pltpu.SemaphoreType.DMA((30,)),
            pltpu.SemaphoreType.DMA((30,)),
            pltpu.SemaphoreType.DMA((seq,)),
            pltpu.SemaphoreType.DMA((seq,)),
            pltpu.SemaphoreType.DMA((slates,)),
            pltpu.SemaphoreType.DMA((slates,)),
        ],
        compiler_params=pltpu.CompilerParams(
            collective_id=0, has_side_effects=True, vmem_limit_bytes=56 * 2**20
        ),
        name="slate_attention",
    )(
        features[0],
        personal,
        labels,
        gain_in[None],
        w_query,
        w_key,
        w_value,
        w_out,
        gain_out[None],
        w_score[None],
    )
    return (mixed[None], scores, loss[0, 0])


def solution(mesh):
    return jax.shard_map(
        shards,
        mesh=mesh,
        in_specs=(
            P("slate", "seq", None),
            P("slate"),
            P("slate", "seq"),
            P(),
            P(),
            P(),
            P(),
            P(),
            P(),
            P(),
            P(),
        ),
        out_specs=(P("slate", "seq", None), P("slate", "seq"), P()),
        check_vma=False,
    )
```

```python
import functools

import jax
import jax.numpy as jnp
from jax import lax
from jax.experimental import pallas as pl
from jax.experimental.pallas import tpu as pltpu
from jax.sharding import PartitionSpec as P

HEADS = 8
soft_cap = 20.0
norm_eps = 1e-06

bf16, f32 = jnp.bfloat16, jnp.float32
LOG2E = 1.4426950408889634
BLOCK = 256
AHEAD = 3
MESH = pl.DeviceIdType.MESH


def capped_weight(products):
    return jnp.exp2(jnp.tanh(products * (128.0 / 8 / soft_cap)) * (soft_cap * LOG2E))


def project_keys(rows, wk, k_ref):
    keys = jnp.dot(rows, wk, preferred_element_type=f32).astype(bf16)
    for pair in range(2):
        k_ref[pair] = keys[:, pair * 128 : (pair + 1) * 128]


def project_values(rows, wv_t, vt_ref):
    values_t = lax.dot_general(
        wv_t, rows, (((1,), (1,)), ((), ())), preferred_element_type=f32
    ).astype(bf16)
    for head in range(4):
        vt_ref[head, 0:64, :] = values_t[head * 64 : (head + 1) * 64]


def project_queries(rows, wq_t, qt_ref, at):
    queries_t = lax.dot_general(
        wq_t, rows, (((1,), (1,)), ((), ())), preferred_element_type=f32
    ).astype(bf16) * bf16(1.0 / 128)
    count = rows.shape[0]
    for head in range(4):
        mine, other = (head % 2) * 64, 64 - (head % 2) * 64
        qt_ref[head, mine : mine + 64, at : at + count] = queries_t[head * 64 : (head + 1) * 64]
        qt_ref[head, other : other + 64, at : at + count] = jnp.zeros((64, count), bf16)


def attend(k_refs, vt_refs, qt_ref, o_ref, heads, tiles):
    kts = k_refs[0].shape[1] // BLOCK
    work = [(g, h, t, b) for g in range(2) for h in heads for t in tiles for b in range(kts)]
    ready = {}
    total = None
    for i in range(len(work) + AHEAD):
        if i < len(work):
            g, h, t, b = work[i]
            products = jnp.dot(
                k_refs[g][h // 2, b * BLOCK : (b + 1) * BLOCK],
                qt_ref[h, :, t * BLOCK : (t + 1) * BLOCK],
                preferred_element_type=f32,
            )
            ready[i] = capped_weight(products).astype(bf16)
        if i >= AHEAD:
            g, h, t, b = work[i - AHEAD]
            part = jnp.dot(
                vt_refs[g][h, :, b * BLOCK : (b + 1) * BLOCK],
                ready.pop(i - AHEAD),
                preferred_element_type=f32,
            )
            total = part if b == 0 else total + part
            if b == kts - 1:
                o_ref[h, :, t * BLOCK : (t + 1) * BLOCK] += total


def rms_scale(rows):
    return lax.rsqrt(jnp.mean(rows * rows, axis=-1, keepdims=True) + norm_eps)


def fused_kernel(
    seq,
    slates,
    features_ref,
    personal_ref,
    labels_ref,
    gain_in_ref,
    wq_ref,
    wk_ref,
    wv_ref,
    wo_ref,
    gain_out_ref,
    w_score_ref,
    mixed_ref,
    scores_ref,
    loss_ref,
    x_ref,
    k_a_ref,
    k_b_ref,
    vt_a_ref,
    vt_b_ref,
    qt_ref,
    o_ref,
    give_ref,
    att_ref,
    wvt_ref,
    sum_ref,
    parts_ref,
    losses_ref,
    send_sem,
    recv_sem,
    parts_send,
    parts_recv,
    losses_send,
    losses_recv,
):
    rows, width = features_ref.shape
    half = width // 2
    third = rows // 3
    me = lax.axis_index("seq")
    my_slate = lax.axis_index("slate")
    core, x, z = lax.rem(me, 2), lax.rem(lax.div(me, 2), 4), lax.div(me, 8)
    at = lambda zz, xx, cc: (zz * 4 + xx) * 2 + cc
    right = at(z, lax.rem(x + 1, 4), core)
    left = at(z, lax.rem(x + 3, 4), core)
    across = at(1 - z, x, core)
    partner = at(z, x, 1 - core)

    barrier = pltpu.get_barrier_semaphore()
    for k in range(1, seq):
        pl.semaphore_signal(
            barrier, inc=1, device_id={"seq": lax.rem(me + k, seq)}, device_id_type=MESH
        )
    for k in range(1, slates):
        pl.semaphore_signal(
            barrier, inc=1, device_id={"slate": lax.rem(my_slate + k, slates)}, device_id_type=MESH
        )

    for t in range(3):
        tile = slice(t * third, (t + 1) * third)
        hidden = features_ref[tile].astype(f32) + personal_ref[...].astype(f32)
        x_ref[0, tile] = (hidden * rms_scale(hidden) * gain_in_ref[...]).astype(bf16)

    copies = {}

    def piece(group, part):
        return x_ref.at[group, part * third : (part + 1) * third]

    def copy(name, source, target, device):
        index = len(copies)
        copies[name] = pltpu.make_async_remote_copy(
            src_ref=source,
            dst_ref=target,
            send_sem=send_sem.at[index],
            recv_sem=recv_sem.at[index],
            device_id={"seq": device},
            device_id_type=MESH,
        )

    copy("own", x_ref.at[0], x_ref.at[1], partner)
    for p in range(3):
        copy(f"a{p}", piece(0, p), piece(2 + p, 0), across)
        copy(f"l{p}", piece(0, p), piece(2 + p, 1), right)
        copy(f"r{p}", piece(0, p), piece(2 + p, 2), left)
        copy(f"al{p}", piece(2 + p, 0), piece(8 + p, 1), right)
        copy(f"ar{p}", piece(2 + p, 0), piece(8 + p, 2), left)
        if p != 1:
            copy(f"o{p}", piece(2 + p, 1), piece(8 + p, 0), right)
        else:
            copy(f"o{p}", piece(2 + p, 2), piece(8 + p, 0), left)
        copy(f"ao{p}", piece(8 + p, 0), piece(14, p), across)
        copy(f"m{p}", x_ref.at[2 + p], x_ref.at[5 + p], partner)
        copy(f"n{p}", x_ref.at[8 + p], x_ref.at[11 + p], partner)
    copy("last", x_ref.at[14], x_ref.at[15], partner)
    copy("swap", give_ref, att_ref.at[core], partner)

    def start(*names):
        for name in names:
            copies[name].start()

    def arrived(*names):
        for name in names:
            copies[name].wait_recv()

    pl.semaphore_wait(barrier, seq - 1 + slates - 1)
    start("own")
    for p in range(3):
        start(f"a{p}", f"l{p}", f"r{p}")

    columns = pl.ds(pl.multiple_of(core * half, half), half)
    wq_t = wq_ref[:, columns].T
    wvt_ref[...] = wv_ref[:, columns].T
    row = lax.broadcasted_iota(jnp.int32, (16, rows), 0)
    k_refs, vt_refs = (k_a_ref, k_b_ref), (vt_a_ref, vt_b_ref)
    for vt_ref, head in [(v, h) for v in vt_refs for h in range(4)]:
        vt_ref[head, 64:80, :] = jnp.where(row == 0, 1.0, 0.0).astype(bf16)
    o_ref[...] = jnp.zeros_like(o_ref)
    project_queries(x_ref[0], wq_t, qt_ref, 0)
    arrived("own")
    project_queries(x_ref[1], wq_t, qt_ref, rows)

    def pair(i, carry):
        @pl.when(i == 1)
        def _():
            for p in (0, 1):
                arrived(f"a{p}", f"l{p}", f"r{p}")
                start(f"al{p}", f"ar{p}", f"o{p}", f"m{p}")

        @pl.when(i == 2)
        def _():
            arrived("a2", "l2", "r2", "m0")
            start("al2", "ar2", "o2", "m2")

        @pl.when(i == 3)
        def _():
            arrived("m1", "m2")
            for p in (0, 1):
                arrived(f"o{p}")
                start(f"ao{p}")

        @pl.when(i == 4)
        def _():
            for p in (0, 1):
                arrived(f"al{p}", f"ar{p}")
                start(f"n{p}")
            arrived("o2")
            start("ao2")

        @pl.when(i == 5)
        def _():
            arrived("al2", "ar2", "n0")
            start("n2")

        @pl.when(i == 6)
        def _():
            arrived("n1", "n2", "ao0", "ao1", "ao2")
            start("last")

        @pl.when(i == 7)
        def _():
            arrived("last")

        for b in range(2):
            project_keys(x_ref[2 * i + b], wk_ref[:, columns], k_refs[b])
            project_values(x_ref[2 * i + b], wvt_ref[...], vt_refs[b])
        tiles = range(qt_ref.shape[2] // BLOCK)
        attend(k_refs, vt_refs, qt_ref, o_ref, range(4), tiles)
        return carry

    lax.fori_loop(0, seq // 2, pair, 0)

    def finished(head, first):
        span = slice(first, first + rows)
        return (o_ref[head, 0:64, span] * (1.0 / o_ref[head, 64:65, span])).astype(bf16)

    for head in range(4):
        give_ref[head * 64 : (head + 1) * 64] = finished(head, rows)
    start("swap")
    for head in range(4):
        att_ref[core, head * 64 : (head + 1) * 64] = finished(head, 0)

    def projected(c, tile):
        return lax.dot_general(
            att_ref[c, :, tile],
            wo_ref[pl.ds(pl.multiple_of(c * half, half), half)],
            (((0,), (0,)), ((), ())),
            preferred_element_type=f32,
        )

    for t in range(3):
        tile = slice(t * third, (t + 1) * third)
        hidden = features_ref[tile].astype(f32) + personal_ref[...].astype(f32)
        sum_ref[tile] = hidden + projected(core, tile)
    arrived("swap")

    sums = [jnp.zeros((1, third), f32)] * 3
    for t in range(3):
        tile = slice(t * third, (t + 1) * third)
        mixed = sum_ref[tile] + projected(1 - core, tile)
        mixed_ref[tile] = mixed.astype(bf16)
        scored = jnp.sum(
            mixed * rms_scale(mixed) * gain_out_ref[...] * w_score_ref[...], axis=-1, keepdims=True
        )
        scored = jnp.broadcast_to(scored, (third, 128)).T[0:1]
        scores_ref[:, tile] = scored
        weight = jnp.exp(labels_ref[:, tile].astype(f32))
        terms = (jnp.exp(scored), weight, weight * scored)
        sums = [total + term for total, term in zip(sums, terms)]

    def shared(tile, buffer, sends, recvs, axis, mine, count):
        buffer[mine] = tile
        sent = []
        for k in range(1, count):
            sent.append(
                pltpu.make_async_remote_copy(
                    src_ref=buffer.at[mine],
                    dst_ref=buffer.at[mine],
                    send_sem=sends.at[k],
                    recv_sem=recvs.at[mine],
                    device_id={axis: lax.rem(mine + k, count)},
                    device_id_type=MESH,
                )
            )
            sent[-1].start()
        for k in range(1, count):
            other = lax.rem(mine + k, count)
            pltpu.make_async_remote_copy(
                src_ref=buffer.at[other],
                dst_ref=buffer.at[other],
                send_sem=sends.at[k],
                recv_sem=recvs.at[other],
                device_id={axis: other},
                device_id_type=MESH,
            ).wait_recv()
        total = buffer[0]
        for k in range(1, count):
            total = total + buffer[k]
        for one in sent:
            one.wait_send()
        return total

    row = lax.broadcasted_iota(jnp.int32, (8, 128), 0)
    tile = jnp.zeros((8, 128), f32)
    for i, total in enumerate(sums):
        tile = jnp.where(row == i, jnp.sum(total, axis=-1, keepdims=True), tile)
    tile = shared(tile, parts_ref, parts_send, parts_recv, "seq", me, seq)
    slate_loss = jnp.log(tile[0:1] / float(rows * seq)) - tile[2:3] / tile[1:2]
    slate_loss = jnp.broadcast_to(slate_loss, (8, 128))
    loss_ref[...] = shared(
        slate_loss, losses_ref, losses_send, losses_recv, "slate", my_slate, slates
    )[0:1, 0:1]
    for one in copies.values():
        one.wait_send()


def shards(
    features,
    user_ids,
    labels,
    user_table,
    gain_in,
    w_query,
    w_key,
    w_value,
    w_out,
    gain_out,
    w_score,
):
    _, rows, width = features.shape
    seq, slates = lax.axis_size("seq"), lax.axis_size("slate")
    personal = lax.dynamic_slice_in_dim(user_table, user_ids[0], 1, 0)
    vmem = pl.BlockSpec(memory_space=pltpu.VMEM)
    mixed, scores, loss = pl.pallas_call(
        functools.partial(fused_kernel, seq, slates),
        out_shape=(
            pltpu.VMEM((rows, width), bf16),
            pltpu.VMEM((1, rows), f32),
            jax.ShapeDtypeStruct((1, 1), f32),
        ),
        in_specs=[vmem] * 10,
        out_specs=(vmem, vmem, vmem),
        scratch_shapes=[
            pltpu.VMEM((seq, rows, width), bf16),
            pltpu.VMEM((2, rows, 128), bf16),
            pltpu.VMEM((2, rows, 128), bf16),
            pltpu.VMEM((4, 80, rows), bf16),
            pltpu.VMEM((4, 80, rows), bf16),
            pltpu.VMEM((4, 128, 2 * rows), bf16),
            pltpu.VMEM((4, 80, 2 * rows), f32),
            pltpu.VMEM((width // 2, rows), bf16),
            pltpu.VMEM((2, width // 2, rows), bf16),
            pltpu.VMEM((width // 2, width), bf16),
            pltpu.VMEM((rows, width), f32),
            pltpu.VMEM((seq, 8, 128), f32),
            pltpu.VMEM((slates, 8, 128), f32),
            pltpu.SemaphoreType.DMA((30,)),
            pltpu.SemaphoreType.DMA((30,)),
            pltpu.SemaphoreType.DMA((seq,)),
            pltpu.SemaphoreType.DMA((seq,)),
            pltpu.SemaphoreType.DMA((slates,)),
            pltpu.SemaphoreType.DMA((slates,)),
        ],
        compiler_params=pltpu.CompilerParams(
            collective_id=0,
            has_side_effects=True,
            vmem_limit_bytes=56 * 2**20,
        ),
        name="slate_attention",
    )(
        features[0],
        personal,
        labels,
        gain_in[None],
        w_query,
        w_key,
        w_value,
        w_out,
        gain_out[None],
        w_score[None],
    )
    return (mixed[None], scores, loss[0, 0])


def solution(mesh):
    return jax.shard_map(
        shards,
        mesh=mesh,
        in_specs=(
            P("slate", "seq", None),
            P("slate"),
            P("slate", "seq"),
            P(),
            P(),
            P(),
            P(),
            P(),
            P(),
            P(),
            P(),
        ),
        out_specs=(P("slate", "seq", None), P("slate", "seq"), P()),
        check_vma=False,
    )
```

```python
import functools

import jax
import jax.numpy as jnp
from jax import lax
from jax.experimental import pallas as pl
from jax.experimental.pallas import tpu as pltpu
from jax.sharding import PartitionSpec as P

HEADS = 8
soft_cap = 20.0
norm_eps = 1e-06

bf16, f32 = jnp.bfloat16, jnp.float32
LOG2E = 1.4426950408889634
BLOCK = 256
AHEAD = 3
MESH = pl.DeviceIdType.MESH


def capped_weight(products):
    return jnp.exp2(jnp.tanh(products * (128.0 / 8 / soft_cap)) * (soft_cap * LOG2E))


def project_keys(rows, wk, k_ref):
    keys = jnp.dot(rows, wk, preferred_element_type=f32).astype(bf16)
    for pair in range(2):
        k_ref[pair] = keys[:, pair * 128 : (pair + 1) * 128]


def project_values(rows, wv_t, vt_ref):
    values_t = lax.dot_general(
        wv_t, rows, (((1,), (1,)), ((), ())), preferred_element_type=f32
    ).astype(bf16)
    for head in range(4):
        vt_ref[head, 0:64, :] = values_t[head * 64 : (head + 1) * 64]


def project_queries(rows, wq_t, qt_ref, at):
    queries_t = lax.dot_general(
        wq_t, rows, (((1,), (1,)), ((), ())), preferred_element_type=f32
    ).astype(bf16) * bf16(1.0 / 128)
    count = rows.shape[0]
    for head in range(4):
        mine, other = (head % 2) * 64, 64 - (head % 2) * 64
        qt_ref[head, mine : mine + 64, at : at + count] = queries_t[head * 64 : (head + 1) * 64]
        qt_ref[head, other : other + 64, at : at + count] = jnp.zeros((64, count), bf16)


def attend(k_refs, vt_refs, qt_ref, o_ref, heads, tiles, second, following):
    kts = k_refs[0].shape[1] // BLOCK
    work = [(g, h, t, b) for g in range(2) for h in heads for t in tiles for b in range(kts)]
    ready = {}
    total = None
    for i in range(len(work) + AHEAD):
        if i == len(work) // 8:
            second()
        if i == len(work) * 5 // 8:
            following()
        if i < len(work):
            g, h, t, b = work[i]
            products = jnp.dot(
                k_refs[g][h // 2, b * BLOCK : (b + 1) * BLOCK],
                qt_ref[h, :, t * BLOCK : (t + 1) * BLOCK],
                preferred_element_type=f32,
            )
            ready[i] = capped_weight(products).astype(bf16)
        if i >= AHEAD:
            g, h, t, b = work[i - AHEAD]
            part = jnp.dot(
                vt_refs[g][h, :, b * BLOCK : (b + 1) * BLOCK],
                ready.pop(i - AHEAD),
                preferred_element_type=f32,
            )
            total = part if b == 0 else total + part
            if b == kts - 1:
                o_ref[h, :, t * BLOCK : (t + 1) * BLOCK] += total


def rms_scale(rows):
    return lax.rsqrt(jnp.mean(rows * rows, axis=-1, keepdims=True) + norm_eps)


def fused_kernel(
    seq,
    slates,
    features_ref,
    personal_ref,
    labels_ref,
    gain_in_ref,
    wq_ref,
    wk_ref,
    wv_ref,
    wo_ref,
    gain_out_ref,
    w_score_ref,
    mixed_ref,
    scores_ref,
    loss_ref,
    x_ref,
    k_a_ref,
    k_b_ref,
    vt_a_ref,
    vt_b_ref,
    qt_ref,
    o_ref,
    give_ref,
    att_ref,
    wvt_ref,
    sum_ref,
    parts_ref,
    losses_ref,
    send_sem,
    recv_sem,
    parts_send,
    parts_recv,
    losses_send,
    losses_recv,
):
    rows, width = features_ref.shape
    half = width // 2
    third = rows // 3
    me = lax.axis_index("seq")
    my_slate = lax.axis_index("slate")
    core, x, z = lax.rem(me, 2), lax.rem(lax.div(me, 2), 4), lax.div(me, 8)
    at = lambda zz, xx, cc: (zz * 4 + xx) * 2 + cc
    right = at(z, lax.rem(x + 1, 4), core)
    left = at(z, lax.rem(x + 3, 4), core)
    across = at(1 - z, x, core)
    partner = at(z, x, 1 - core)

    barrier = pltpu.get_barrier_semaphore()
    for k in range(1, seq):
        pl.semaphore_signal(
            barrier, inc=1, device_id={"seq": lax.rem(me + k, seq)}, device_id_type=MESH
        )
    for k in range(1, slates):
        pl.semaphore_signal(
            barrier, inc=1, device_id={"slate": lax.rem(my_slate + k, slates)}, device_id_type=MESH
        )

    for t in range(3):
        tile = slice(t * third, (t + 1) * third)
        hidden = features_ref[tile].astype(f32) + personal_ref[...].astype(f32)
        x_ref[0, tile] = (hidden * rms_scale(hidden) * gain_in_ref[...]).astype(bf16)

    copies = {}

    def piece(group, part):
        return x_ref.at[group, part * third : (part + 1) * third]

    def copy(name, source, target, device):
        index = len(copies)
        copies[name] = pltpu.make_async_remote_copy(
            src_ref=source,
            dst_ref=target,
            send_sem=send_sem.at[index],
            recv_sem=recv_sem.at[index],
            device_id={"seq": device},
            device_id_type=MESH,
        )

    copy("own", x_ref.at[0], x_ref.at[1], partner)
    for p in range(3):
        copy(f"a{p}", piece(0, p), piece(2 + p, 0), across)
        copy(f"l{p}", piece(0, p), piece(2 + p, 1), right)
        copy(f"r{p}", piece(0, p), piece(2 + p, 2), left)
        copy(f"al{p}", piece(2 + p, 0), piece(8 + p, 1), right)
        copy(f"ar{p}", piece(2 + p, 0), piece(8 + p, 2), left)
        if p != 1:
            copy(f"o{p}", piece(2 + p, 1), piece(8 + p, 0), right)
        else:
            copy(f"o{p}", piece(2 + p, 2), piece(8 + p, 0), left)
        copy(f"ao{p}", piece(8 + p, 0), piece(14, p), across)
        copy(f"m{p}", x_ref.at[2 + p], x_ref.at[5 + p], partner)
        copy(f"n{p}", x_ref.at[8 + p], x_ref.at[11 + p], partner)
    copy("last", x_ref.at[14], x_ref.at[15], partner)
    copy("swap", give_ref, att_ref.at[core], partner)

    def start(*names):
        for name in names:
            copies[name].start()

    def arrived(*names):
        for name in names:
            copies[name].wait_recv()

    pl.semaphore_wait(barrier, seq - 1 + slates - 1)
    start("own")
    for p in range(3):
        start(f"a{p}", f"l{p}", f"r{p}")

    columns = pl.ds(pl.multiple_of(core * half, half), half)
    wq_t = wq_ref[:, columns].T
    wvt_ref[...] = wv_ref[:, columns].T
    row = lax.broadcasted_iota(jnp.int32, (16, rows), 0)
    k_refs, vt_refs = (k_a_ref, k_b_ref), (vt_a_ref, vt_b_ref)
    for vt_ref, head in [(v, h) for v in vt_refs for h in range(4)]:
        vt_ref[head, 64:80, :] = jnp.where(row == 0, 1.0, 0.0).astype(bf16)
    o_ref[...] = jnp.zeros_like(o_ref)
    project_queries(x_ref[0], wq_t, qt_ref, 0)

    def project(g, b):
        project_keys(x_ref[g], wk_ref[:, columns], k_refs[b])
        project_values(x_ref[g], wvt_ref[...], vt_refs[b])

    project(0, 0)
    arrived("own")
    project_queries(x_ref[1], wq_t, qt_ref, rows)

    def pair(i, carry):
        @pl.when(i == 1)
        def _():
            for p in (0, 1):
                arrived(f"a{p}", f"l{p}", f"r{p}")
                start(f"al{p}", f"ar{p}", f"o{p}", f"m{p}")
            project(2, 0)

        @pl.when(i == 2)
        def _():
            arrived("a2", "l2", "r2")
            start("al2", "ar2", "o2", "m2")
            arrived("m0", "m1")
            project(4, 0)

        @pl.when(i == 3)
        def _():
            arrived("m2", "o0", "al0", "ar0")
            start("ao0", "n0")

        @pl.when(i == 4)
        def _():
            for p in (1, 2):
                arrived(f"o{p}", f"al{p}", f"ar{p}")
                start(f"ao{p}", f"n{p}")

        @pl.when(i == 5)
        def _():
            arrived("n0", "n1")

        @pl.when(i == 6)
        def _():
            arrived("n2", "ao0", "ao1", "ao2")
            start("last")

        @pl.when(i == 7)
        def _():
            arrived("last")

        late = lax.div(i + 5, 7)
        following = lax.rem(1 + late * (2 * i + 1), seq)
        attend(
            k_refs,
            vt_refs,
            qt_ref,
            o_ref,
            range(4),
            range(qt_ref.shape[2] // BLOCK),
            lambda: project(2 * i + 1, 1),
            lambda: project(following, 0),
        )
        return carry

    lax.fori_loop(0, seq // 2, pair, 0)

    def finished(head, first):
        span = slice(first, first + rows)
        return (o_ref[head, 0:64, span] * (1.0 / o_ref[head, 64:65, span])).astype(bf16)

    for head in range(4):
        give_ref[head * 64 : (head + 1) * 64] = finished(head, rows)
    start("swap")
    for head in range(4):
        att_ref[core, head * 64 : (head + 1) * 64] = finished(head, 0)

    def projected(c, tile):
        return lax.dot_general(
            att_ref[c, :, tile],
            wo_ref[pl.ds(pl.multiple_of(c * half, half), half)],
            (((0,), (0,)), ((), ())),
            preferred_element_type=f32,
        )

    for t in range(3):
        tile = slice(t * third, (t + 1) * third)
        hidden = features_ref[tile].astype(f32) + personal_ref[...].astype(f32)
        sum_ref[tile] = hidden + projected(core, tile)
    arrived("swap")

    sums = [jnp.zeros((1, third), f32)] * 3
    for t in range(3):
        tile = slice(t * third, (t + 1) * third)
        mixed = sum_ref[tile] + projected(1 - core, tile)
        mixed_ref[tile] = mixed.astype(bf16)
        scored = jnp.sum(
            mixed * rms_scale(mixed) * gain_out_ref[...] * w_score_ref[...], axis=-1, keepdims=True
        )
        scored = jnp.broadcast_to(scored, (third, 128)).T[0:1]
        scores_ref[:, tile] = scored
        weight = jnp.exp(labels_ref[:, tile].astype(f32))
        terms = (jnp.exp(scored), weight, weight * scored)
        sums = [total + term for total, term in zip(sums, terms)]

    def shared(tile, buffer, sends, recvs, axis, mine, count):
        buffer[mine] = tile
        sent = []
        for k in range(1, count):
            sent.append(
                pltpu.make_async_remote_copy(
                    src_ref=buffer.at[mine],
                    dst_ref=buffer.at[mine],
                    send_sem=sends.at[k],
                    recv_sem=recvs.at[mine],
                    device_id={axis: lax.rem(mine + k, count)},
                    device_id_type=MESH,
                )
            )
            sent[-1].start()
        for k in range(1, count):
            other = lax.rem(mine + k, count)
            pltpu.make_async_remote_copy(
                src_ref=buffer.at[other],
                dst_ref=buffer.at[other],
                send_sem=sends.at[k],
                recv_sem=recvs.at[other],
                device_id={axis: other},
                device_id_type=MESH,
            ).wait_recv()
        total = buffer[0]
        for k in range(1, count):
            total = total + buffer[k]
        for one in sent:
            one.wait_send()
        return total

    row = lax.broadcasted_iota(jnp.int32, (8, 128), 0)
    tile = jnp.zeros((8, 128), f32)
    for i, total in enumerate(sums):
        tile = jnp.where(row == i, jnp.sum(total, axis=-1, keepdims=True), tile)
    tile = shared(tile, parts_ref, parts_send, parts_recv, "seq", me, seq)
    slate_loss = jnp.log(tile[0:1] / float(rows * seq)) - tile[2:3] / tile[1:2]
    slate_loss = jnp.broadcast_to(slate_loss, (8, 128))
    loss_ref[...] = shared(
        slate_loss, losses_ref, losses_send, losses_recv, "slate", my_slate, slates
    )[0:1, 0:1]
    for one in copies.values():
        one.wait_send()


def shards(
    features,
    user_ids,
    labels,
    user_table,
    gain_in,
    w_query,
    w_key,
    w_value,
    w_out,
    gain_out,
    w_score,
):
    _, rows, width = features.shape
    seq, slates = lax.axis_size("seq"), lax.axis_size("slate")
    personal = lax.dynamic_slice_in_dim(user_table, user_ids[0], 1, 0)
    vmem = pl.BlockSpec(memory_space=pltpu.VMEM)
    mixed, scores, loss = pl.pallas_call(
        functools.partial(fused_kernel, seq, slates),
        out_shape=(
            pltpu.VMEM((rows, width), bf16),
            pltpu.VMEM((1, rows), f32),
            jax.ShapeDtypeStruct((1, 1), f32),
        ),
        in_specs=[vmem] * 10,
        out_specs=(vmem, vmem, vmem),
        scratch_shapes=[
            pltpu.VMEM((seq, rows, width), bf16),
            pltpu.VMEM((2, rows, 128), bf16),
            pltpu.VMEM((2, rows, 128), bf16),
            pltpu.VMEM((4, 80, rows), bf16),
            pltpu.VMEM((4, 80, rows), bf16),
            pltpu.VMEM((4, 128, 2 * rows), bf16),
            pltpu.VMEM((4, 80, 2 * rows), f32),
            pltpu.VMEM((width // 2, rows), bf16),
            pltpu.VMEM((2, width // 2, rows), bf16),
            pltpu.VMEM((width // 2, width), bf16),
            pltpu.VMEM((rows, width), f32),
            pltpu.VMEM((seq, 8, 128), f32),
            pltpu.VMEM((slates, 8, 128), f32),
            pltpu.SemaphoreType.DMA((30,)),
            pltpu.SemaphoreType.DMA((30,)),
            pltpu.SemaphoreType.DMA((seq,)),
            pltpu.SemaphoreType.DMA((seq,)),
            pltpu.SemaphoreType.DMA((slates,)),
            pltpu.SemaphoreType.DMA((slates,)),
        ],
        compiler_params=pltpu.CompilerParams(
            collective_id=0,
            has_side_effects=True,
            vmem_limit_bytes=56 * 2**20,
        ),
        name="slate_attention",
    )(
        features[0],
        personal,
        labels,
        gain_in[None],
        w_query,
        w_key,
        w_value,
        w_out,
        gain_out[None],
        w_score[None],
    )
    return (mixed[None], scores, loss[0, 0])


def solution(mesh):
    return jax.shard_map(
        shards,
        mesh=mesh,
        in_specs=(
            P("slate", "seq", None),
            P("slate"),
            P("slate", "seq"),
            P(),
            P(),
            P(),
            P(),
            P(),
            P(),
            P(),
            P(),
        ),
        out_specs=(P("slate", "seq", None), P("slate", "seq"), P()),
        check_vma=False,
    )
```
